32 devices in a mesh: row: 4 (over y, x), col: 8 (over z, core).
Axes of the slice: x: 2, y: 2, z: 4, core: 2. Of those that a mesh axis runs over, the one named last changes fastest.
Arguments:
- spectra: bfloat16 [16, 2048, 2048], P('row', None, 'col'), may hold values from -6 to 6
- coupling: float32 [16], replicated, may hold values from 0.2 to 1
Outputs:
- returned_spectra: bfloat16 [16, 2048, 2048], P('row', None, 'col')
The draws below stay inside these ranges and needn't reach their ends.
All inputs are finite; a program needn't handle non-finite values.
Results may differ from the reference program's by a relative error of at most 0.0079.
Values may be sent and summed in bfloat16 or wider, within the bound.
No kernel may reach another device: no remote copies, remote signals or barrier semaphores. Data moves between devices by JAX's collectives and lax.ppermute only.
A program may use at most 128 MiB of HBM per device.

```python
import math
import jax
import jax.numpy as jnp
from jax import lax

FIELDS = 8
LEV = 2
NX = 3072
NY = 3072
M = 1024


def shard_levels(own_key, dims, split, least, high):
    gain, own = 1.0, jax.random.fold_in(own_key, 6)
    for dim, blocks in split:
        heights = jnp.exp(jax.random.uniform(jax.random.fold_in(own, dim), (blocks,), jnp.float32, least / len(split), high / len(split)))
        gain = gain * jnp.repeat(heights, dims[dim] // blocks).reshape([-1 if axis == dim else 1 for axis in range(len(dims))])
    return gain


def scatter_about(stream_key, dims, scale, limit, shards=(), kind=jnp.bfloat16):
    array = scale * jax.random.normal(stream_key, dims, jnp.float32)
    if shards:
        array = array * shard_levels(stream_key, dims, shards, -0.22, 0.18)
    return jnp.clip(array, -limit, limit).astype(kind)


def setup_inputs(seed: int = 0) -> dict:
    seeds = jax.random.split(jax.random.key(seed), 3)
    spectra = scatter_about(seeds[0], (FIELDS * LEV, 2 * M, 2 * M), 1.0, 6.0, ((0, 4), (2, 8)))
    coupling = jnp.clip(jnp.exp(jax.random.uniform(seeds[1], (FIELDS * LEV,), jnp.float32, math.log(0.2), math.log(1.0))), 0.2, 1.0)
    return dict(spectra=spectra, coupling=coupling)


def fourier_rows(mode_count, length, factor):
    wavenumber = jnp.arange(1, mode_count + 1, dtype=jnp.int32)
    position = jnp.arange(length, dtype=jnp.int32)
    residue = wavenumber[:, None] * position[None, :] % length
    angles = residue.astype(jnp.float32) * (2.0 * math.pi / length)
    table = jnp.concatenate([jnp.cos(angles), jnp.sin(angles)], 0) * factor
    return table.astype(jnp.bfloat16)

def ellipse(row_index, column_index, mode_count):
    row_waves = row_index % mode_count + 1
    col_waves = column_index % mode_count + 1
    inside = row_waves[:, None] * row_waves[:, None] + col_waves[None, :] * col_waves[None, :] <= mode_count * mode_count
    return inside.astype(jnp.float32)

def reference(spectra, coupling):
    inverse_y = fourier_rows(M, NY, 1.0 / math.sqrt(M)).T
    inverse_x = fourier_rows(M, NX, 1.0 / math.sqrt(M))
    forward_x = fourier_rows(M, NX, 2.0 * math.sqrt(M) / NX).T
    forward_y = fourier_rows(M, NY, 2.0 * math.sqrt(M) / NY)
    modes = jnp.arange(2 * M, dtype=jnp.int32)
    inside = ellipse(modes, modes, M)

    def one_field(bundle):
        spectrum, strength = bundle
        half_done = jnp.dot(inverse_y, spectrum, preferred_element_type=jnp.float32).astype(jnp.bfloat16)
        gridded = jnp.dot(half_done, inverse_x, preferred_element_type=jnp.float32)
        tendency = (gridded + strength * gridded * gridded).astype(jnp.bfloat16)
        projected = jnp.dot(tendency, forward_x, preferred_element_type=jnp.float32).astype(jnp.bfloat16)
        result = jnp.dot(forward_y, projected, preferred_element_type=jnp.float32)
        return (result * inside).astype(jnp.bfloat16)
    return lax.map(one_field, (spectra, coupling))
```

```python
import math

import jax
import jax.numpy as jnp
from jax import lax
from jax.experimental import pallas as pl
from jax.experimental.pallas import tpu as pltpu
from jax.sharding import PartitionSpec as P


NX = 3072
NY = 3072
STEP = 16
EDGE = 64
TILE = 256
BLOCKS = 4
VMEM_MIB = {"inverse_y": 16}
VMEM_MOST = 63
LEVELS = 3


def angle_pair(left, right, length):
    residue = (left[:, None] * right[None, :]) % length
    angles = residue.astype(jnp.float32) * (2.0 * math.pi / length)
    return jnp.cos(angles), jnp.sin(angles)


def dot(a, b):
    return jnp.dot(a, b, preferred_element_type=jnp.float32)


def whole(shape):
    return pl.BlockSpec(shape, lambda *_: (0,) * len(shape))


def call(body, outs, grid, ins, in_specs, out_specs, flops, moved, name, scalars=(), scratch=(), **more):
    return pl.pallas_call(
        body,
        out_shape=outs,
        grid_spec=pltpu.PrefetchScalarGridSpec(
            num_scalar_prefetch=len(scalars),
            grid=grid,
            in_specs=in_specs,
            out_specs=out_specs,
            scratch_shapes=scratch,
        ),
        cost_estimate=pl.CostEstimate(flops=flops, bytes_accessed=moved, transcendentals=0),
        compiler_params=pltpu.CompilerParams(vmem_limit_bytes=VMEM_MIB.get(name, VMEM_MOST) * 2**20),
        **more,
    )(*scalars, *ins)


def pick(cosine, base_cos, base_sin):
    return jnp.where(cosine, base_cos, base_sin), jnp.where(cosine, -base_sin, base_cos)


def spread(first, second, fine_cos, fine_sin, scale):
    return ((first * fine_cos + second * fine_sin) * scale).astype(jnp.bfloat16)


def inverse_x_tables(base, fine, kinds, blocks, width, scale):
    span = fine[0].shape[1]
    count = kinds.shape[0]

    def body(kinds_ref, blocks_ref, cos_ref, sin_ref, fine_cos, fine_sin, out_ref):
        first, second = pick(kinds_ref[pl.program_id(0)] > 0, cos_ref[...], sin_ref[...])
        fine_c, fine_s = fine_cos[...] * scale, fine_sin[...] * scale
        for a in range(width // STEP):
            lines = spread(first[a : a + 1], second[a : a + 1], fine_c, fine_s, 1.0)
            for j in range(span // TILE):
                out_ref[j, a * STEP : (a + 1) * STEP] = lines[:, j * TILE : (j + 1) * TILE]

    rows = pl.BlockSpec((width // STEP, span), lambda i, k, b: (b[i], 0))
    return call(
        body,
        jax.ShapeDtypeStruct((span // TILE, count * width, TILE), jnp.bfloat16),
        (count,),
        (*base, *fine),
        [rows, rows, whole((STEP, span)), whole((STEP, span))],
        pl.BlockSpec((span // TILE, width, TILE), lambda i, k, b: (0, i, 0)),
        4 * count * width * span,
        2 * count * width * span,
        "tables_ix",
        (kinds, blocks),
    )


def forward_y_tables(base, fine, member, members, share, modes):
    order = [member ^ s for s in range(members)]
    weight = (2.0 * math.sqrt(modes) / NY) * jnp.where(jnp.arange(base[0].shape[1]) == 0, 1.0, 2.0)[None]
    lines = (*base, *fine, weight)
    block = share
    if share % 128:
        lines = [
            jnp.concatenate([lax.dynamic_slice_in_dim(a, o * share, share, 1) for o in order], axis=1) for a in lines
        ]
        order, block = [jnp.zeros((), jnp.int32)], members * share

    def body(order_ref, cos_ref, sin_ref, fine_cos, fine_sin, weight_ref, out_ref):
        cosine = pl.program_id(0) == 0
        fine_c, fine_s, scale = fine_cos[...], fine_sin[...], weight_ref[...]
        for a in range(modes // STEP):
            first, second = pick(cosine, cos_ref[a : a + 1], sin_ref[a : a + 1])
            out_ref[a * STEP : (a + 1) * STEP] = spread(first, second, fine_c, fine_s, scale)

    def part(height):
        return pl.BlockSpec((height, block), lambda h, s, o: (0, o[s]))

    return call(
        body,
        jax.ShapeDtypeStruct((2 * modes, members * share), jnp.bfloat16),
        (2, len(order)),
        lines,
        [part(a.shape[0]) for a in lines],
        pl.BlockSpec((modes, block), lambda h, s, o: (h, s)),
        8 * modes * members * share,
        4 * modes * members * share,
        "tables_fy",
        (jnp.stack(order),),
    )


def forward_x_tables(base, fine, kinds, blocks, width, modes):
    steps = base[0].shape[0]
    count = kinds.shape[0]
    unit = 2.0 * math.sqrt(modes) / NX

    def body(kinds_ref, blocks_ref, cos_ref, sin_ref, fine_cos, fine_sin, out_ref):
        cosine = kinds_ref[pl.program_id(0)] > 0
        fine_c, fine_s = fine_cos[...], fine_sin[...]
        for a in range(steps):
            first, second = pick(cosine, cos_ref[a : a + 1], sin_ref[a : a + 1])
            scale = 2.0 * unit
            if a == 0 or (a + 1) * STEP > NX // 2:
                point = lax.broadcasted_iota(jnp.int32, (STEP, 1), 0) + a * STEP
                ends = (point == 0) | (point == NX // 2)
                scale = unit * jnp.where(ends, 1.0, jnp.where(point > NX // 2, 0.0, 2.0))
            out_ref[a * STEP : (a + 1) * STEP] = spread(first, second, fine_c, fine_s, scale)

    rows = pl.BlockSpec((steps, width), lambda i, k, b: (0, b[i]))
    thin = pl.BlockSpec((STEP, width), lambda i, k, b: (0, b[i]))
    return call(
        body,
        jax.ShapeDtypeStruct((steps * STEP, count * width), jnp.bfloat16),
        (count,),
        (*base, *fine),
        [rows, rows, thin, thin],
        pl.BlockSpec((steps * STEP, width), lambda i, k, b: (0, i)),
        4 * steps * STEP * count * width,
        2 * steps * STEP * count * width,
        "tables_fx",
        (kinds, blocks),
    )


def inverse_y_table(base, fine, member, share, modes):
    rows = 2 * share + EDGE
    scale = 1.0 / math.sqrt(modes)

    def body(member_ref, cos_ref, sin_ref, fine_cos, fine_sin, out_ref):
        start = member_ref[0] * (share // STEP)
        fine_c, fine_s = fine_cos[...], fine_sin[...]
        for a in range(share // STEP):
            base_cos, base_sin = cos_ref[pl.ds(start + a, 1)], sin_ref[pl.ds(start + a, 1)]
            out_ref[a * STEP : (a + 1) * STEP] = spread(base_cos, -base_sin, fine_c, fine_s, scale)
            low = share + EDGE + a * STEP
            out_ref[low : low + STEP] = spread(base_sin, base_cos, fine_c, fine_s, scale)
        edge = NY // 2 // STEP
        for a in range(EDGE // STEP):
            low = share + a * STEP
            out_ref[low : low + STEP] = spread(
                cos_ref[edge : edge + 1], -sin_ref[edge : edge + 1], fine_c, fine_s, scale
            )

    return call(
        body,
        jax.ShapeDtypeStruct((rows, modes), jnp.bfloat16),
        (1,),
        (*base, *fine),
        [whole(a.shape) for a in (*base, *fine)],
        whole((rows, modes)),
        4 * rows * modes,
        2 * rows * modes,
        "tables_iy",
        (member[None],),
    )


def inverse_y(table, piece, share):
    modes = table.shape[1]
    rows, width = table.shape[0], piece.shape[1]
    top, step = share + EDGE, rows // BLOCKS

    def body(*refs):
        even_ref, odd_ref, out_ref = refs[BLOCKS:]
        for j in range(BLOCKS):
            low = j * step
            cut = min(max(top - low, 0), step)
            if cut:
                out_ref[low : low + cut] = dot(refs[j][:cut], even_ref[...]).astype(jnp.bfloat16)
            if cut < step:
                out_ref[low + cut : low + step] = dot(refs[j][cut:], odd_ref[...]).astype(jnp.bfloat16)

    def part(shape, j):
        return pl.BlockSpec(shape, lambda i: (j, 0))

    return call(
        body,
        jax.ShapeDtypeStruct((rows, width), jnp.bfloat16),
        (1,),
        (*[table] * BLOCKS, piece, piece),
        [part((step, modes), j) for j in range(BLOCKS)] + [part((modes, width), j) for j in range(2)],
        whole((rows, width)),
        2 * rows * modes * width,
        2 * (rows * modes + 2 * modes * width + rows * width),
        "inverse_y",
    )


def inverse_x(lines, table, part):
    rows, width = lines[0].shape
    tiles = table.shape[0]
    count = len(lines)

    def body(*refs):
        table_ref, out_ref = refs[count], refs[count + 1]
        lines_here = jnp.concatenate([r[...] for r in refs[:count]], axis=1)
        out_ref[0] = dot(lines_here, table_ref[0]).astype(jnp.bfloat16)

    return call(
        body,
        jax.ShapeDtypeStruct((tiles, rows, TILE), jnp.bfloat16),
        (tiles,),
        (*lines, table),
        [whole((rows, width))] * count + [pl.BlockSpec((1, count * width, TILE), lambda i: (i, part, 0))],
        pl.BlockSpec((1, rows, TILE), lambda i: (i, 0, 0)),
        2 * rows * count * width * tiles * TILE,
        4 * rows * tiles * TILE,
        "inverse_x",
    )


def grid_term(lines, table, part, mine, table_back, turn, members, strength, sign, share):
    rows, width = lines[0].shape
    tiles = table.shape[0]
    count = len(lines)
    top = share + EDGE
    chunk = share // 2

    def body(*refs):
        strength_ref, sign_ref = refs[:2]
        line_refs = refs[2 : 2 + count]
        table_ref, mine_ref, back_ref, mine_out, other_out = refs[2 + count : 7 + count]
        out_refs, kept_ref = refs[7 + count : -1], refs[-1]
        c, s = strength_ref[0], sign_ref[0]
        step = pl.program_id(0)

        def other(*parts):
            picked = [jnp.concatenate([r[low : low + size] for low, size in parts], axis=0) for r in line_refs]
            return dot(jnp.concatenate(picked, axis=1), table_ref[0])

        def put(ref, low, value):
            ref[0, low : low + value.shape[0]] = value.astype(jnp.bfloat16)

        @pl.when(step < tiles)
        def _():
            for low in range(0, share, chunk):
                both = other((low, chunk), (top + low, chunk))
                x, y = both[:chunk], both[chunk:]
                a = mine_ref[0, low : low + chunk].astype(jnp.float32)
                b = mine_ref[0, top + low : top + low + chunk].astype(jnp.float32)
                p, q, u, v = a + x, b + y, a - x, b - y
                sums, gaps = (p * p + q * q) * (0.5 * c), (u * u + v * v) * (0.5 * c * s)
                cross, skew = (p * q) * c, (u * v) * (c * s)
                put(other_out, low, x + (sums - gaps))
                put(other_out, top + low, y + (cross - skew))
                put(mine_out, low, a + (sums + gaps))
                put(mine_out, top + low, b + (cross + skew))
            x, a = other((share, EDGE)), mine_ref[0, share:top].astype(jnp.float32)
            p, u = a + x, a - x
            sums, gaps = (p * p) * (0.5 * c), (u * u) * (0.5 * c * s)
            put(other_out, share, x + (sums - gaps))
            put(mine_out, share, a + (sums + gaps))
            kept_ref[step] = other_out[0]

        for j, out_ref in enumerate(out_refs):

            @pl.when(step == tiles + j)
            def _():
                points = jnp.concatenate([kept_ref[k] for k in range(tiles)], axis=1)
                out_ref[...] = dot(points, back_ref[...]).astype(jnp.bfloat16)

    def clip(i):
        return jnp.minimum(i, tiles - 1)

    def owner(i, *_):
        return (0, turn * members + lax.rem(jnp.clip(i - tiles, 0, members - 1) + 1, members))

    tile = pl.BlockSpec((1, rows, TILE), lambda i, *_: (clip(i), 0, 0))
    mine, other, *parts = call(
        body,
        [jax.ShapeDtypeStruct((tiles, rows, TILE), jnp.bfloat16)] * 2
        + [jax.ShapeDtypeStruct((rows, width), jnp.bfloat16)] * members,
        (tiles + members,),
        (*lines, table, mine, table_back),
        [whole((rows, width))] * count
        + [
            pl.BlockSpec((1, count * width, TILE), lambda i, *_: (clip(i), part, 0)),
            tile,
            pl.BlockSpec((tiles * TILE, width), owner),
        ],
        [tile, tile] + [whole((rows, width))] * members,
        2 * rows * (count + members) * width * tiles * TILE,
        8 * rows * tiles * TILE,
        "grid_term",
        (strength, sign),
        scratch=[pltpu.VMEM((tiles, rows, TILE), jnp.bfloat16)],
    )
    return mine, other, parts[-1:] + parts[:-1]


def forward_x(sources, table_back, pieces, width):
    tiles, rows = sources[0].shape[:2]
    count = len(sources)

    def body(*refs):
        table_ref, out_refs = refs[1 + tiles * count], refs[2 + tiles * count :]
        for j, (source, _) in enumerate(pieces):

            @pl.when(pl.program_id(0) == j)
            def _():
                first = 1 + source * tiles
                points = jnp.concatenate([refs[first + k][0] for k in range(tiles)], axis=1)
                out_refs[j][...] = dot(points, table_ref[...]).astype(jnp.bfloat16)

    def tile(k):
        return pl.BlockSpec((1, rows, TILE), lambda i, c: (k, 0, 0), pipeline_mode=pl.Buffered(1))

    return call(
        body,
        [jax.ShapeDtypeStruct((rows, width), jnp.bfloat16)] * len(pieces),
        (len(pieces),),
        (*[s for s in sources for _ in range(tiles)], table_back),
        [tile(k) for _ in sources for k in range(tiles)]
        + [pl.BlockSpec((tiles * TILE, width), lambda i, c: (0, c[i]))],
        [whole((rows, width))] * len(pieces),
        2 * rows * tiles * TILE * len(pieces) * width,
        2 * count * rows * tiles * TILE,
        "forward_x",
        (jnp.array([column for _, column in pieces], jnp.int32),),
    )


def forward_y(lines, table, column_start, slot, share, bounds, fields=0):
    width = lines[0].shape[1]
    modes = table.shape[0] // 2
    top = share + EDGE
    count = len(lines)

    def body(*refs):
        where_ref, table_refs = refs[0], refs[1 + count : 1 + count + BLOCKS]
        out_refs = refs[1 + count + BLOCKS :]
        half = pl.program_id(0)
        low = pl.multiple_of(half * top, STEP)
        points = jnp.concatenate([r[pl.ds(low, share)] for r in refs[1 : 1 + count]], axis=0)
        total = jnp.concatenate([dot(r[...], points) for r in table_refs], axis=0)
        waves = lax.broadcasted_iota(jnp.int32, (modes, 1), 0) + 1
        unit = jnp.where(half == 0, 2.0 * math.sqrt(modes) / NY, 0.0)
        nyquist = jnp.where(waves % 2 == 1, -unit, unit).astype(jnp.bfloat16).astype(jnp.float32)
        total += nyquist * refs[1][share : share + 1].astype(jnp.float32)
        across = lax.broadcasted_iota(jnp.int32, (1, width), 1) + where_ref[0] + 1
        inside = waves * waves <= modes * modes - across * across
        total = jnp.where(inside, total, 0.0).astype(jnp.bfloat16)
        if fields:
            out_refs[0][0] = total
        else:
            for out_ref, start, stop in zip(out_refs, bounds[:-1], bounds[1:]):
                out_ref[0] = total[start:stop]

    def fetch(j):
        return pl.BlockSpec((modes // BLOCKS, count * share), lambda i, s: (BLOCKS * i + j, 0))

    if fields:
        outs = jax.ShapeDtypeStruct((fields, 2 * modes, width), jnp.bfloat16)
        out_specs = pl.BlockSpec((1, modes, width), lambda i, s: (s[1], i, 0))
    else:
        sizes = [high - low for low, high in zip(bounds[:-1], bounds[1:])]
        outs = [jax.ShapeDtypeStruct((2, n, width), jnp.bfloat16) for n in sizes]
        out_specs = [pl.BlockSpec((1, n, width), lambda i, s: (i, 0, 0)) for n in sizes]
    return call(
        body,
        outs,
        (2,),
        (*lines, *[table] * BLOCKS),
        [whole(lines[0].shape)] * count + [fetch(j) for j in range(BLOCKS)],
        out_specs,
        4 * modes * share * count * width,
        2 * (2 * modes * share * count + 2 * modes * width),
        "forward_y",
        (jnp.stack([column_start, slot]),),
    )


def place(result, blocks, bounds, slot):
    _, height, width = result.shape
    modes = height // 2
    count = len(blocks)

    def body(*refs):
        out_ref = refs[-1]
        for j in range(count):
            out_ref[0, bounds[j] : bounds[j + 1]] = refs[1 + j][0]

    return call(
        body,
        jax.ShapeDtypeStruct(result.shape, result.dtype),
        (2,),
        (*blocks, result),
        [pl.BlockSpec((1, *b.shape[1:]), lambda i, s: (i, 0, 0)) for b in blocks] + [pl.BlockSpec(memory_space=pl.ANY)],
        pl.BlockSpec((1, modes, width), lambda i, s: (s[0], i, 0)),
        height * width,
        4 * height * width,
        "place",
        (slot[None],),
        input_output_aliases={1 + count: 0},
    )


def row_limits(modes, width, devices):
    limits = []
    for c in range(devices):
        low = (c * width) % modes + 1
        limits.append(min(modes, -(-math.isqrt(modes * modes - low * low) // 16) * 16))
    return limits


def round_trip(devices, spectra, coupling):
    fields, height, width = spectra.shape
    modes = height // 2
    members = devices // fields
    share = NY // 2 // members
    span = NX // 2 + TILE
    half = fields // 2
    me = lax.axis_index("col")
    group, member = me // members, me % members
    first_field = lax.axis_index("row") * fields
    strength = lax.dynamic_slice_in_dim(coupling, first_field + group, 1)
    is_mine = group < half
    sign = jnp.where(is_mine, 1.0, -1.0)[None]

    def send(piece, turn, shift, chosen=None):
        partners = []
        for c in range(devices):
            there = ((c // members) ^ turn) * members + ((c % members) ^ shift)
            if chosen is None or there in chosen:
                partners.append((c, there))
        return lax.ppermute(piece, "col", partners)

    pieces = [lax.dynamic_index_in_dim(spectra, group ^ t, 0, keepdims=False) for t in range(fields)]
    arrived = [pieces[0]] + [send(pieces[t], t, 0) for t in range(1, fields)]

    def ints(n, by=1):
        return jnp.arange(n, dtype=jnp.int32) * by

    by_mode = angle_pair(ints(modes // STEP, STEP) + 1, ints(span), NX) + angle_pair(ints(STEP), ints(span), NX)
    by_point = angle_pair(ints(span // STEP, STEP), ints(modes) + 1, NX) + angle_pair(ints(STEP), ints(modes) + 1, NX)
    by_mode, by_point = lax.optimization_barrier((by_mode, by_point))
    owners = jnp.stack([(group ^ t) * members + (member ^ s) for t in range(fields) for s in range(members)])
    kinds = (owners * width < modes).astype(jnp.int32)
    blocks = owners % (modes // width)
    table_y = inverse_y_table(by_point[:2], by_point[2:], member, share, modes)
    table_x = inverse_x_tables(by_mode[:2], by_mode[2:], kinds, blocks, width, 1.0 / math.sqrt(modes))
    table_back_x = forward_x_tables(by_point[:2], by_point[2:], kinds, blocks, width, modes)
    table_back_y = forward_y_tables(by_mode[:2], by_mode[2:], member, members, share, modes)

    lines = []
    for t in range(fields):
        for s in range(members):
            piece = arrived[t] if s == 0 else send(arrived[t], 0, s)
            lines.append(inverse_y(table_y, piece, share))
    cut = half * members
    mine = inverse_x(lines[:cut], table_x, 0)
    order = turns(fields)
    mine, other, parts = grid_term(
        lines[cut:], table_x, 1, mine, table_back_x, order[0], members, strength, sign, share
    )

    limits = row_limits(modes, width, devices)
    levels = sorted(set(limits))
    while len(levels) > LEVELS:
        gaps = [(levels[i + 1] - levels[i], i) for i in range(len(levels) - 1)]
        levels.pop(min(gaps)[1])
    bounds = [0] + levels
    bounds[-1] = modes

    returned, result, ready, batches = {}, None, {}, back_batches(fields)
    for t in order:
        for later in batches:
            if t == later[0]:
                kinds_here = sorted({u >= half for u in later})
                flat = forward_x(
                    [(mine, other)[k] for k in kinds_here],
                    table_back_x,
                    [(kinds_here.index(u >= half), u * members + s) for u in later for s in [*range(1, members), 0]],
                    width,
                )
                ready.update({u: flat[j * members : (j + 1) * members] for j, u in enumerate(later)})
        if t in ready:
            parts = ready[t][-1:] + ready[t][:-1]
        rows = [parts[0]] + [send(parts[s], 0, s) for s in range(1, members)]
        start = (((group ^ t) * members + member) * width) % modes
        cuts = bounds if t > 1 else [0, modes]
        sums = forward_y(rows, table_back_y, start, group, share, cuts, fields if t == 0 else 0)
        if t == 0:
            result = sums
        else:
            returned[t] = [
                send(b, t, 0, [c for c in range(devices) if limits[c] > cuts[j]])
                for j, b in enumerate(sums)
            ]
    for t, parts in returned.items():
        result = place(result, parts, bounds if t > 1 else [0, modes], group ^ t)
    return result


def turns(fields):
    return [fields - 1, *range(1, fields - 1), 0]


def back_batches(fields):
    return [turns(fields)[1:]]


def solution(mesh):
    placed = (P("row", None, "col"), P())
    devices = mesh.shape["col"]

    def body(spectra, coupling):
        return round_trip(devices, spectra, coupling)

    return jax.shard_map(body, mesh=mesh, in_specs=placed, out_specs=P("row", None, "col"), check_vma=False)
```

```python
import math

import jax
import jax.numpy as jnp
from jax import lax
from jax.experimental import pallas as pl
from jax.experimental.pallas import tpu as pltpu
from jax.sharding import PartitionSpec as P


NX = 3072
NY = 3072
STEP = 16
EDGE = 64
TILE = 256
BLOCKS = 4
VMEM_MIB = {"inverse_y": 16}
VMEM_MOST = 63
LEVELS = 3


def angle_pair(left, right, length):
    residue = (left[:, None] * right[None, :]) % length
    angles = residue.astype(jnp.float32) * (2.0 * math.pi / length)
    return jnp.cos(angles), jnp.sin(angles)


def dot(a, b):
    return jnp.dot(a, b, preferred_element_type=jnp.float32)


def whole(shape):
    return pl.BlockSpec(shape, lambda *_: (0,) * len(shape))


def call(body, outs, grid, ins, in_specs, out_specs, flops, moved, name, scalars=(), scratch=(), **more):
    return pl.pallas_call(
        body,
        out_shape=outs,
        grid_spec=pltpu.PrefetchScalarGridSpec(
            num_scalar_prefetch=len(scalars),
            grid=grid,
            in_specs=in_specs,
            out_specs=out_specs,
            scratch_shapes=scratch,
        ),
        cost_estimate=pl.CostEstimate(flops=flops, bytes_accessed=moved, transcendentals=0),
        compiler_params=pltpu.CompilerParams(vmem_limit_bytes=VMEM_MIB.get(name, VMEM_MOST) * 2**20),
        **more,
    )(*scalars, *ins)


def pick(cosine, base_cos, base_sin):
    return jnp.where(cosine, base_cos, base_sin), jnp.where(cosine, -base_sin, base_cos)


def spread(first, second, fine_cos, fine_sin, scale):
    return ((first * fine_cos + second * fine_sin) * scale).astype(jnp.bfloat16)


def inverse_x_tables(base, fine, kinds, blocks, width, scale):
    span = fine[0].shape[1]
    count = kinds.shape[0]

    def body(kinds_ref, blocks_ref, cos_ref, sin_ref, fine_cos, fine_sin, out_ref):
        first, second = pick(kinds_ref[pl.program_id(0)] > 0, cos_ref[...], sin_ref[...])
        fine_c, fine_s = fine_cos[...] * scale, fine_sin[...] * scale
        for a in range(width // STEP):
            lines = spread(first[a : a + 1], second[a : a + 1], fine_c, fine_s, 1.0)
            for j in range(span // TILE):
                out_ref[j, a * STEP : (a + 1) * STEP] = lines[:, j * TILE : (j + 1) * TILE]

    rows = pl.BlockSpec((width // STEP, span), lambda i, k, b: (b[i], 0))
    return call(
        body,
        jax.ShapeDtypeStruct((span // TILE, count * width, TILE), jnp.bfloat16),
        (count,),
        (*base, *fine),
        [rows, rows, whole((STEP, span)), whole((STEP, span))],
        pl.BlockSpec((span // TILE, width, TILE), lambda i, k, b: (0, i, 0)),
        4 * count * width * span,
        2 * count * width * span,
        "tables_ix",
        (kinds, blocks),
    )


def forward_y_tables(base, fine, member, members, share, modes):
    order = [member ^ s for s in range(members)]
    weight = (2.0 * math.sqrt(modes) / NY) * jnp.where(jnp.arange(base[0].shape[1]) == 0, 1.0, 2.0)[None]
    lines = (*base, *fine, weight)
    block = share
    if share % 128:
        lines = [
            jnp.concatenate([lax.dynamic_slice_in_dim(a, o * share, share, 1) for o in order], axis=1) for a in lines
        ]
        order, block = [jnp.zeros((), jnp.int32)], members * share

    def body(order_ref, cos_ref, sin_ref, fine_cos, fine_sin, weight_ref, out_ref):
        cosine = pl.program_id(0) == 0
        fine_c, fine_s, scale = fine_cos[...], fine_sin[...], weight_ref[...]
        for a in range(modes // STEP):
            first, second = pick(cosine, cos_ref[a : a + 1], sin_ref[a : a + 1])
            out_ref[a * STEP : (a + 1) * STEP] = spread(first, second, fine_c, fine_s, scale)

    def part(height):
        return pl.BlockSpec((height, block), lambda h, s, o: (0, o[s]))

    return call(
        body,
        jax.ShapeDtypeStruct((2 * modes, members * share), jnp.bfloat16),
        (2, len(order)),
        lines,
        [part(a.shape[0]) for a in lines],
        pl.BlockSpec((modes, block), lambda h, s, o: (h, s)),
        8 * modes * members * share,
        4 * modes * members * share,
        "tables_fy",
        (jnp.stack(order),),
    )


def forward_x_tables(base, fine, kinds, blocks, width, modes):
    steps = base[0].shape[0]
    count = kinds.shape[0]
    unit = 2.0 * math.sqrt(modes) / NX

    def body(kinds_ref, blocks_ref, cos_ref, sin_ref, fine_cos, fine_sin, out_ref):
        cosine = kinds_ref[pl.program_id(0)] > 0
        fine_c, fine_s = fine_cos[...], fine_sin[...]
        for a in range(steps):
            first, second = pick(cosine, cos_ref[a : a + 1], sin_ref[a : a + 1])
            scale = 2.0 * unit
            if a == 0 or (a + 1) * STEP > NX // 2:
                point = lax.broadcasted_iota(jnp.int32, (STEP, 1), 0) + a * STEP
                ends = (point == 0) | (point == NX // 2)
                scale = unit * jnp.where(ends, 1.0, jnp.where(point > NX // 2, 0.0, 2.0))
            out_ref[a * STEP : (a + 1) * STEP] = spread(first, second, fine_c, fine_s, scale)

    rows = pl.BlockSpec((steps, width), lambda i, k, b: (0, b[i]))
    thin = pl.BlockSpec((STEP, width), lambda i, k, b: (0, b[i]))
    return call(
        body,
        jax.ShapeDtypeStruct((steps * STEP, count * width), jnp.bfloat16),
        (count,),
        (*base, *fine),
        [rows, rows, thin, thin],
        pl.BlockSpec((steps * STEP, width), lambda i, k, b: (0, i)),
        4 * steps * STEP * count * width,
        2 * steps * STEP * count * width,
        "tables_fx",
        (kinds, blocks),
    )


def inverse_y_table(base, fine, member, share, modes):
    rows = 2 * share + EDGE
    scale = 1.0 / math.sqrt(modes)

    def body(member_ref, cos_ref, sin_ref, fine_cos, fine_sin, out_ref):
        start = member_ref[0] * (share // STEP)
        fine_c, fine_s = fine_cos[...], fine_sin[...]
        for a in range(share // STEP):
            base_cos, base_sin = cos_ref[pl.ds(start + a, 1)], sin_ref[pl.ds(start + a, 1)]
            out_ref[a * STEP : (a + 1) * STEP] = spread(base_cos, -base_sin, fine_c, fine_s, scale)
            low = share + EDGE + a * STEP
            out_ref[low : low + STEP] = spread(base_sin, base_cos, fine_c, fine_s, scale)
        edge = NY // 2 // STEP
        for a in range(EDGE // STEP):
            low = share + a * STEP
            out_ref[low : low + STEP] = spread(
                cos_ref[edge : edge + 1], -sin_ref[edge : edge + 1], fine_c, fine_s, scale
            )

    return call(
        body,
        jax.ShapeDtypeStruct((rows, modes), jnp.bfloat16),
        (1,),
        (*base, *fine),
        [whole(a.shape) for a in (*base, *fine)],
        whole((rows, modes)),
        4 * rows * modes,
        2 * rows * modes,
        "tables_iy",
        (member[None],),
    )


def inverse_y(table, piece, share):
    modes = table.shape[1]
    rows, width = table.shape[0], piece.shape[1]
    top, step = share + EDGE, rows // BLOCKS

    def body(*refs):
        even_ref, odd_ref, out_ref = refs[BLOCKS:]
        for j in range(BLOCKS):
            low = j * step
            cut = min(max(top - low, 0), step)
            if cut:
                out_ref[low : low + cut] = dot(refs[j][:cut], even_ref[...]).astype(jnp.bfloat16)
            if cut < step:
                out_ref[low + cut : low + step] = dot(refs[j][cut:], odd_ref[...]).astype(jnp.bfloat16)

    def part(shape, j):
        return pl.BlockSpec(shape, lambda i: (j, 0))

    return call(
        body,
        jax.ShapeDtypeStruct((rows, width), jnp.bfloat16),
        (1,),
        (*[table] * BLOCKS, piece, piece),
        [part((step, modes), j) for j in range(BLOCKS)] + [part((modes, width), j) for j in range(2)],
        whole((rows, width)),
        2 * rows * modes * width,
        2 * (rows * modes + 2 * modes * width + rows * width),
        "inverse_y",
    )


def inverse_x(lines, table, part):
    rows, width = lines[0].shape
    tiles = table.shape[0]
    count = len(lines)

    def body(*refs):
        table_ref, out_ref = refs[count], refs[count + 1]
        lines_here = jnp.concatenate([r[...] for r in refs[:count]], axis=1)
        out_ref[0] = dot(lines_here, table_ref[0]).astype(jnp.bfloat16)

    return call(
        body,
        jax.ShapeDtypeStruct((tiles, rows, TILE), jnp.bfloat16),
        (tiles,),
        (*lines, table),
        [whole((rows, width))] * count + [pl.BlockSpec((1, count * width, TILE), lambda i: (i, part, 0))],
        pl.BlockSpec((1, rows, TILE), lambda i: (i, 0, 0)),
        2 * rows * count * width * tiles * TILE,
        4 * rows * tiles * TILE,
        "inverse_x",
    )


def grid_term(lines, table, part, mine, table_back, turn, members, strength, own_field, sign, share):
    rows, width = lines[0].shape
    tiles = table.shape[0]
    count = len(lines)
    top = share + EDGE
    chunk = share // 4

    def body(*refs):
        strength_ref, field_ref, sign_ref = refs[:3]
        line_refs = refs[3 : 3 + count]
        table_ref, mine_ref, back_ref, mine_out, other_out = refs[3 + count : 8 + count]
        out_refs, kept_ref = refs[8 + count : -1], refs[-1]
        c, s = strength_ref[field_ref[0]], sign_ref[0]
        step = pl.program_id(0)

        def other(*parts):
            picked = [jnp.concatenate([r[low : low + size] for low, size in parts], axis=0) for r in line_refs]
            return dot(jnp.concatenate(picked, axis=1), table_ref[0])

        def put(ref, low, value):
            ref[0, low : low + value.shape[0]] = value.astype(jnp.bfloat16)

        @pl.when(step < tiles)
        def _():
            for low in range(0, share, chunk):
                both = other((low, chunk), (top + low, chunk))
                x, y = both[:chunk], both[chunk:]
                a = mine_ref[0, low : low + chunk].astype(jnp.float32)
                b = mine_ref[0, top + low : top + low + chunk].astype(jnp.float32)
                p, q, u, v = a + x, b + y, a - x, b - y
                sums, gaps = (p * p + q * q) * (0.5 * c), (u * u + v * v) * (0.5 * c * s)
                cross, skew = (p * q) * c, (u * v) * (c * s)
                put(other_out, low, x + (sums - gaps))
                put(other_out, top + low, y + (cross - skew))
                put(mine_out, low, a + (sums + gaps))
                put(mine_out, top + low, b + (cross + skew))
            x, a = other((share, EDGE)), mine_ref[0, share:top].astype(jnp.float32)
            p, u = a + x, a - x
            sums, gaps = (p * p) * (0.5 * c), (u * u) * (0.5 * c * s)
            put(other_out, share, x + (sums - gaps))
            put(mine_out, share, a + (sums + gaps))
            kept_ref[step] = other_out[0]

        for j, out_ref in enumerate(out_refs):

            @pl.when(step == tiles + j)
            def _():
                points = jnp.concatenate([kept_ref[k] for k in range(tiles)], axis=1)
                out_ref[...] = dot(points, back_ref[...]).astype(jnp.bfloat16)

    def clip(i):
        return jnp.minimum(i, tiles - 1)

    def owner(i, *_):
        return (0, turn * members + lax.rem(jnp.clip(i - tiles, 0, members - 1) + 1, members))

    tile = pl.BlockSpec((1, rows, TILE), lambda i, *_: (clip(i), 0, 0))
    mine, other, *parts = call(
        body,
        [jax.ShapeDtypeStruct((tiles, rows, TILE), jnp.bfloat16)] * 2
        + [jax.ShapeDtypeStruct((rows, width), jnp.bfloat16)] * members,
        (tiles + members,),
        (*lines, table, mine, table_back),
        [whole((rows, width))] * count
        + [
            pl.BlockSpec((1, count * width, TILE), lambda i, *_: (clip(i), part, 0)),
            tile,
            pl.BlockSpec((tiles * TILE, width), owner),
        ],
        [tile, tile] + [whole((rows, width))] * members,
        2 * rows * (count + members) * width * tiles * TILE,
        8 * rows * tiles * TILE,
        "grid_term",
        (strength, own_field, sign),
        scratch=[pltpu.VMEM((tiles, rows, TILE), jnp.bfloat16)],
    )
    return mine, other, parts[-1:] + parts[:-1]


def forward_x(sources, table_back, owners, members, width):
    tiles, rows = sources[0].shape[:2]
    count, span = len(sources), members * width

    def body(*refs):
        table_refs = refs[count : count + len(owners)]
        out_refs, total_ref = refs[count + len(owners) : -1], refs[-1]

        @pl.when(pl.program_id(0) == 0)
        def _():
            total_ref[...] = jnp.zeros_like(total_ref)

        for j, (source, _) in enumerate(owners):
            total_ref[:, j * span : (j + 1) * span] += dot(refs[source][0], table_refs[j][...])

        @pl.when(pl.program_id(0) == tiles - 1)
        def _():
            for j, out_ref in enumerate(out_refs):
                out_ref[...] = total_ref[:, j * width : (j + 1) * width].astype(jnp.bfloat16)

    def columns(turn):
        return pl.BlockSpec((TILE, span), lambda i: (i, turn))

    return call(
        body,
        [jax.ShapeDtypeStruct((rows, width), jnp.bfloat16)] * (len(owners) * members),
        (tiles,),
        (*sources, *[table_back] * len(owners)),
        [pl.BlockSpec((1, rows, TILE), lambda i: (i, 0, 0))] * count + [columns(turn) for _, turn in owners],
        [whole((rows, width))] * (len(owners) * members),
        2 * rows * tiles * TILE * len(owners) * span,
        2 * count * rows * tiles * TILE,
        "forward_x",
        scratch=[pltpu.VMEM((rows, len(owners) * span), jnp.float32)],
    )


def forward_y(lines, table, column_start, slot, share, bounds, fields=0):
    width = lines[0].shape[1]
    modes = table.shape[0] // 2
    top = share + EDGE
    count = len(lines)

    def body(*refs):
        where_ref, table_refs = refs[0], refs[1 + count : 1 + count + BLOCKS]
        out_refs = refs[1 + count + BLOCKS :]
        half = pl.program_id(0)
        low = pl.multiple_of(half * top, STEP)
        points = jnp.concatenate([r[pl.ds(low, share)] for r in refs[1 : 1 + count]], axis=0)
        total = jnp.concatenate([dot(r[...], points) for r in table_refs], axis=0)
        waves = lax.broadcasted_iota(jnp.int32, (modes, 1), 0) + 1
        unit = jnp.where(half == 0, 2.0 * math.sqrt(modes) / NY, 0.0)
        nyquist = jnp.where(waves % 2 == 1, -unit, unit).astype(jnp.bfloat16).astype(jnp.float32)
        total += nyquist * refs[1][share : share + 1].astype(jnp.float32)
        across = lax.broadcasted_iota(jnp.int32, (1, width), 1) + where_ref[0] + 1
        inside = waves * waves <= modes * modes - across * across
        total = jnp.where(inside, total, 0.0).astype(jnp.bfloat16)
        if fields:
            out_refs[0][0] = total
        else:
            for out_ref, start, stop in zip(out_refs, bounds[:-1], bounds[1:]):
                out_ref[0] = total[start:stop]

    def fetch(j):
        return pl.BlockSpec((modes // BLOCKS, count * share), lambda i, s: (BLOCKS * i + j, 0))

    if fields:
        outs = jax.ShapeDtypeStruct((fields, 2 * modes, width), jnp.bfloat16)
        out_specs = pl.BlockSpec((1, modes, width), lambda i, s: (s[1], i, 0))
    else:
        sizes = [high - low for low, high in zip(bounds[:-1], bounds[1:])]
        outs = [jax.ShapeDtypeStruct((2, n, width), jnp.bfloat16) for n in sizes]
        out_specs = [pl.BlockSpec((1, n, width), lambda i, s: (i, 0, 0)) for n in sizes]
    return call(
        body,
        outs,
        (2,),
        (*lines, *[table] * BLOCKS),
        [whole(lines[0].shape)] * count + [fetch(j) for j in range(BLOCKS)],
        out_specs,
        4 * modes * share * count * width,
        2 * (2 * modes * share * count + 2 * modes * width),
        "forward_y",
        (jnp.stack([column_start, slot]),),
    )


def place(result, blocks, bounds, slot):
    _, height, width = result.shape
    modes = height // 2
    count = len(blocks)

    def body(*refs):
        out_ref = refs[-1]
        for j in range(count):
            out_ref[0, bounds[j] : bounds[j + 1]] = refs[1 + j][0]

    return call(
        body,
        jax.ShapeDtypeStruct(result.shape, result.dtype),
        (2,),
        (*blocks, result),
        [pl.BlockSpec((1, *b.shape[1:]), lambda i, s: (i, 0, 0)) for b in blocks] + [pl.BlockSpec(memory_space=pl.ANY)],
        pl.BlockSpec((1, modes, width), lambda i, s: (s[0], i, 0)),
        height * width,
        4 * height * width,
        "place",
        (slot[None],),
        input_output_aliases={1 + count: 0},
    )


def row_limits(modes, width, devices):
    limits = []
    for c in range(devices):
        low = (c * width) % modes + 1
        limits.append(min(modes, -(-math.isqrt(modes * modes - low * low) // 16) * 16))
    return limits


def round_trip(devices, spectra, coupling):
    fields, height, width = spectra.shape
    modes = height // 2
    members = devices // fields
    share = NY // 2 // members
    span = NX // 2 + TILE
    half = fields // 2
    me = lax.axis_index("col")
    group, member = me // members, me % members
    first_field = lax.axis_index("row") * fields
    own_field = (first_field + group)[None]
    is_mine = group < half
    sign = jnp.where(is_mine, 1.0, -1.0)[None]

    def send(piece, turn, shift, chosen=None):
        partners = []
        for c in range(devices):
            there = ((c // members) ^ turn) * members + ((c % members) ^ shift)
            if chosen is None or there in chosen:
                partners.append((c, there))
        return lax.ppermute(piece, "col", partners)

    first = lax.dynamic_index_in_dim(spectra, group ^ half, 0, keepdims=False)
    first, spectra = lax.optimization_barrier((first, spectra))
    pieces = [
        first if t == half else lax.dynamic_index_in_dim(spectra, group ^ t, 0, keepdims=False) for t in range(fields)
    ]
    arrived = [pieces[0]] + [send(pieces[t], t, 0) for t in range(1, fields)]

    def ints(n, by=1):
        return jnp.arange(n, dtype=jnp.int32) * by

    by_mode = angle_pair(ints(modes // STEP, STEP) + 1, ints(span), NX) + angle_pair(ints(STEP), ints(span), NX)
    by_point = angle_pair(ints(span // STEP, STEP), ints(modes) + 1, NX) + angle_pair(ints(STEP), ints(modes) + 1, NX)
    by_mode, by_point = lax.optimization_barrier((by_mode, by_point))
    owners = jnp.stack([(group ^ t) * members + (member ^ s) for t in range(fields) for s in range(members)])
    kinds = (owners * width < modes).astype(jnp.int32)
    blocks = owners % (modes // width)
    table_y = inverse_y_table(by_point[:2], by_point[2:], member, share, modes)
    table_x = inverse_x_tables(by_mode[:2], by_mode[2:], kinds, blocks, width, 1.0 / math.sqrt(modes))
    table_back_x = forward_x_tables(by_point[:2], by_point[2:], kinds, blocks, width, modes)
    table_back_y = forward_y_tables(by_mode[:2], by_mode[2:], member, members, share, modes)

    lines = []
    for t in range(fields):
        for s in range(members):
            piece = arrived[t] if s == 0 else send(arrived[t], 0, s)
            lines.append(inverse_y(table_y, piece, share))
    cut = half * members
    mine = inverse_x(lines[:cut], table_x, 0)
    order = turns(fields)
    mine, other, parts = grid_term(
        lines[cut:], table_x, 1, mine, table_back_x, order[0], members, coupling, own_field, sign, share
    )

    limits = row_limits(modes, width, devices)
    levels = sorted(set(limits))
    while len(levels) > LEVELS:
        gaps = [(levels[i + 1] - levels[i], i) for i in range(len(levels) - 1)]
        levels.pop(min(gaps)[1])
    bounds = [0] + levels
    bounds[-1] = modes

    returned, result, ready, batches = {}, None, {}, back_batches(fields)
    for t in order:
        for later in batches:
            if t == later[0]:
                kinds_here = sorted({u >= half for u in later})
                flat = forward_x(
                    [(mine, other)[k] for k in kinds_here],
                    table_back_x,
                    [(kinds_here.index(u >= half), u) for u in later],
                    members,
                    width,
                )
                ready.update({u: flat[j * members : (j + 1) * members] for j, u in enumerate(later)})
        if t in ready:
            parts = ready[t]
        rows = [parts[0]] + [send(parts[s], 0, s) for s in range(1, members)]
        start = (((group ^ t) * members + member) * width) % modes
        cuts = bounds if t > 1 else [0, modes]
        sums = forward_y(rows, table_back_y, start, group, share, cuts, fields if t == 0 else 0)
        if t == 0:
            result = sums
        else:
            returned[t] = [
                send(b, t, 0, [c for c in range(devices) if limits[c] > cuts[j]])
                for j, b in enumerate(sums)
            ]
    for t, parts in returned.items():
        result = place(result, parts, bounds if t > 1 else [0, modes], group ^ t)
    return result


def turns(fields):
    return [fields - 1, *range(1, fields - 1), 0]


def back_batches(fields):
    return [b for b in (turns(fields)[1:-1], [0]) if b]


def solution(mesh):
    placed = (P("row", None, "col"), P())
    devices = mesh.shape["col"]

    def body(spectra, coupling):
        return round_trip(devices, spectra, coupling)

    return jax.shard_map(body, mesh=mesh, in_specs=placed, out_specs=P("row", None, "col"), check_vma=False)
```
